32 devices in a mesh: dp: 4 (over z), shard: 8 (over y, x, core).
Axes of the slice: x: 2, y: 2, z: 4, core: 2. Of those that a mesh axis runs over, the one named last changes fastest.
Arguments:
- token_ids: int32 [64, 1024], P(('dp', 'shard')), may hold values from 0 to 49151
- seq_lengths: int32 [64], P(('dp', 'shard')), may hold values from 256 to 768, as said below
- completion_mask: int32 [64, 1024], P(('dp', 'shard')), may hold values from 0 to 1, as said below
- deal: int32 [64], P(('dp', 'shard')), may hold values from 0 to 15, as said below
- attend_in: float32 [960, 1600], P('shard'), may hold values from -0.1875 to 0.1875
- attend_out: float32 [960, 960], P('shard'), may hold values from -0.25 to 0.25
- feed_in: float32 [960, 5120], P('shard'), may hold values from -0.1875 to 0.1875
- feed_out: float32 [2560, 960], P('shard'), may hold values from -0.046875 to 0.046875
- norm_gains: float32 [3, 960], P(None, 'shard'), may hold values from 0.5 to 1.5
- embed_table: float32 [49152, 960], P(('dp', 'shard')), may hold values from -1 to 1
- attend_in_first: float32 [960, 1600], P('shard'), may hold values from -7.6293945e-06 to 7.6293945e-06
- attend_out_first: float32 [960, 960], P('shard'), may hold values from -7.6293945e-06 to 7.6293945e-06
- feed_in_first: float32 [960, 5120], P('shard'), may hold values from -7.6293945e-06 to 7.6293945e-06
- feed_out_first: float32 [2560, 960], P('shard'), may hold values from -7.6293945e-06 to 7.6293945e-06
- norm_gains_first: float32 [3, 960], P(None, 'shard'), may hold values from -7.6293945e-06 to 7.6293945e-06
- embed_table_first: float32 [49152, 960], P(('dp', 'shard')), may hold values from -7.6293945e-06 to 7.6293945e-06
- attend_in_second: float32 [960, 1600], P('shard'), may hold values from 1.7537952e-12 to 7.015181e-12
- attend_out_second: float32 [960, 960], P('shard'), may hold values from 1.7537952e-12 to 7.015181e-12
- feed_in_second: float32 [960, 5120], P('shard'), may hold values from 1.7537952e-12 to 7.015181e-12
- feed_out_second: float32 [2560, 960], P('shard'), may hold values from 1.7537952e-12 to 7.015181e-12
- norm_gains_second: float32 [3, 960], P(None, 'shard'), may hold values from 1.7537952e-12 to 7.015181e-12
- embed_table_second: float32 [49152, 960], P(('dp', 'shard')), may hold values from 1.7537952e-12 to 7.015181e-12
Outputs:
- new_attend_in: float32 [960, 1600], P('shard')
- new_attend_out: float32 [960, 960], P('shard')
- new_feed_in: float32 [960, 5120], P('shard')
- new_feed_out: float32 [2560, 960], P('shard')
- norm_gains_update: float32 [3, 960], P(None, 'shard')
- new_embed_table: float32 [49152, 960], P(('dp', 'shard'))
- new_attend_in_first: float32 [960, 1600], P('shard')
- new_attend_out_first: float32 [960, 960], P('shard')
- new_feed_in_first: float32 [960, 5120], P('shard')
- new_feed_out_first: float32 [2560, 960], P('shard')
- new_norm_gains_first: float32 [3, 960], P(None, 'shard')
- new_embed_table_first: float32 [49152, 960], P(('dp', 'shard'))
- new_attend_in_second: float32 [960, 1600], P('shard')
- new_attend_out_second: float32 [960, 960], P('shard')
- new_feed_in_second: float32 [960, 5120], P('shard')
- new_feed_out_second: float32 [2560, 960], P('shard')
- new_norm_gains_second: float32 [3, 960], P(None, 'shard')
- new_embed_table_second: float32 [49152, 960], P(('dp', 'shard'))
- mean_loss: float32 [], replicated
- grad_norm: float32 [], replicated
- seq_loss: float32 [64], P(('dp', 'shard'))
The draws below stay inside these ranges and needn't reach their ends.
Inputs may be any that keep to these rules, and one draw needn't show every extreme that they name: `seq_lengths`: the sequences at packed places 2b and 2b + 1 have lengths summing to exactly 1024; in every draw some sequence has 256 tokens and its partner the rest. `completion_mask`: each input slot holds exactly 16 ones, all at positions t with 1024 - length <= t <= 1022 of that slot's sequence. On the 16 sequences of each index of dp (consecutive in input order), deal is a permutation.
All inputs are finite; a program needn't handle non-finite values.
Results may differ from the reference program's by a relative error of at most 0.009.
The reference program's roundings to bfloat16 on the way count: a program that leaves them out, or rounds other values in their place, can miss the bound.
Values may be sent and summed in bfloat16 or wider, within the bound.
A program may use at most 384 MiB of HBM per device.

```python
import math
import jax
import jax.numpy as jnp
import numpy as np
from jax import lax

D = 960
HEADS = 15
KV_HEADS = 5
HEAD_DIM = 64
FF = 2560
VOCAB = 49152
SLOT = 1024
COMP = 16
STEP = 3
SEQS = 64
GROUP_SEQS = 16
COUNT = 1024
KVD = 320
QKV = 1600
PARAMS = 9833280


def shared_layout(key):
    base_key = jax.random.fold_in(key, 7)
    length_key, spot_key, score_key, order_key = jax.random.split(base_key, 4)
    pair_count = SEQS // 2
    group_count = SEQS // GROUP_SEQS
    first_len = jax.random.randint(length_key, (pair_count,), SLOT // 4, SLOT - SLOT // 4 + 1)
    shortest = jax.random.randint(spot_key, (), 0, pair_count)
    first_len = jnp.where(jnp.arange(pair_count) == shortest, SLOT // 4, first_len).astype(jnp.int32)
    packed_len = jnp.stack([first_len, SLOT - first_len], axis=1).reshape(SEQS)
    order_keys = jax.random.split(order_key, group_count)
    orders = jax.vmap(lambda one_key: jax.random.permutation(one_key, GROUP_SEQS))(order_keys).astype(jnp.int32)
    places = jnp.broadcast_to(jnp.arange(GROUP_SEQS, dtype=jnp.int32)[None, :], (group_count, GROUP_SEQS))
    deal = jnp.zeros((group_count, GROUP_SEQS), jnp.int32).at[jnp.arange(group_count)[:, None], orders].set(places)
    deal = deal.reshape(SEQS)
    group_base = jnp.arange(SEQS, dtype=jnp.int32) // GROUP_SEQS * GROUP_SEQS
    lengths = jnp.take(packed_len, group_base + deal).astype(jnp.int32)
    step_ids = jnp.arange(SLOT, dtype=jnp.int32)
    usable = (step_ids[None, :] >= SLOT - lengths[:, None]) & (step_ids[None, :] <= SLOT - 2)
    scores = jax.random.randint(score_key, (SEQS, SLOT), 0, 1 << 20) * SLOT + step_ids[None, :]
    scores = jnp.where(usable, scores, -1)
    _, picked = lax.top_k(scores, COMP)
    marks = jnp.zeros((SEQS, SLOT), jnp.int32).at[jnp.arange(SEQS)[:, None], picked].set(1)
    return (lengths, marks, deal)


def draw_seq_lengths(key, part):
    return shared_layout(key)[0]


def draw_completion_mask(key, part):
    return shared_layout(key)[1]


def draw_deal(key, part):
    return shared_layout(key)[2]


def with_ends(values, own_key, least, largest):
    spot = [jax.random.randint(jax.random.fold_in(own_key, axis), (), 0, length) for axis, length in enumerate(values.shape)]
    longest = values.shape.index(max(values.shape))
    next_to = spot[:longest] + [(spot[longest] + 1) % values.shape[longest]] + spot[longest + 1:]
    return values.at[tuple(spot)].set(least).at[tuple(next_to)].set(largest)


def shard_levels(key, shape, cuts, low, top_value):
    factor_of, own = 1.0, jax.random.fold_in(key, 6)
    for axis_at, shards_of in cuts:
        draws = jnp.exp(jax.random.uniform(jax.random.fold_in(own, axis_at), (shards_of,), jnp.float32, low / len(cuts), top_value / len(cuts)))
        factor_of = factor_of * jnp.repeat(draws, shape[axis_at] // shards_of).reshape([-1 if axis == axis_at else 1 for axis in range(len(shape))])
    return factor_of


def rank_bounds(count, slope):
    portions = [(1 << 20) // math.isqrt(rank ** slope) + 1 for rank in range(1, count + 1)]
    spread = 1 + sum(portions) // (1 << 30)
    return np.cumsum(np.array([max(1, weight // spread) for weight in portions]))


def ranked(stream_key, dims, number_of, lean):
    grid = rank_bounds(number_of, lean)
    lot = jax.random.randint(jax.random.fold_in(stream_key, 1), dims, 0, int(grid[number_of - 1]))
    grade = jnp.searchsorted(jnp.asarray(grid, jnp.int32), lot, side="right")
    return jax.random.permutation(jax.random.fold_in(stream_key, 2), number_of)[grade].astype(jnp.int32)


def gaussian(key, extent, scale, bound, shards=(), held_as=jnp.bfloat16):
    drawn = scale * jax.random.normal(key, extent, jnp.float32)
    if shards:
        drawn = drawn * shard_levels(key, extent, shards, -0.22, 0.18)
    return jnp.clip(drawn, -bound, bound).astype(held_as)


def setup_inputs(seed: int = 0) -> dict:
    streams_of = jax.random.split(jax.random.key(seed), 23)
    token_ids = with_ends(ranked(streams_of[0], (SEQS, SLOT), VOCAB, 2), jax.random.fold_in(streams_of[0], 3), 0, VOCAB - 1).astype(jnp.int32)
    seq_lengths = draw_seq_lengths(jax.random.fold_in(streams_of[22], 71), 0)
    completion_mask = draw_completion_mask(jax.random.fold_in(streams_of[22], 71), 0)
    deal = draw_deal(jax.random.fold_in(streams_of[22], 71), 0)
    attend_in = gaussian(streams_of[4], (D, QKV), D ** -0.5, 0.1875, ((0, 8),), jnp.float32)
    attend_out = gaussian(streams_of[5], (D, D), (D // 2) ** -0.5, 0.25, ((0, 8),), jnp.float32)
    feed_in = gaussian(streams_of[6], (D, 2 * FF), D ** -0.5, 0.1875, ((0, 8),), jnp.float32)
    feed_out = gaussian(streams_of[7], (FF, D), 0.003, 0.046875, ((0, 8),), jnp.float32)
    norm_gains = jnp.clip(1.0 + 0.1 * jax.random.normal(streams_of[8], (3, D), jnp.float32), 0.5, 1.5)
    embed_table = gaussian(streams_of[9], (VOCAB, D), 0.065, 1.0, ((0, 32),), jnp.float32)
    attend_in_first = gaussian(streams_of[10], (D, QKV), (0.01 / (PARAMS + VOCAB * D) ** 0.5), 7.62939453125e-06, ((0, 8),), jnp.float32)
    attend_out_first = gaussian(streams_of[11], (D, D), (0.01 / (PARAMS + VOCAB * D) ** 0.5), 7.62939453125e-06, ((0, 8),), jnp.float32)
    feed_in_first = gaussian(streams_of[12], (D, 2 * FF), (0.01 / (PARAMS + VOCAB * D) ** 0.5), 7.62939453125e-06, ((0, 8),), jnp.float32)
    feed_out_first = gaussian(streams_of[13], (FF, D), (0.01 / (PARAMS + VOCAB * D) ** 0.5), 7.62939453125e-06, ((0, 8),), jnp.float32)
    norm_gains_first = gaussian(streams_of[14], (3, D), (0.01 / (PARAMS + VOCAB * D) ** 0.5), 7.62939453125e-06, ((1, 8),), jnp.float32)
    embed_table_first = gaussian(streams_of[15], (VOCAB, D), (0.01 / (PARAMS + VOCAB * D) ** 0.5), 7.62939453125e-06, ((0, 32),), jnp.float32)
    attend_in_second = jnp.clip(jnp.exp(math.log(7.0151809708485224e-12) - 1.3862944 * jax.random.uniform(streams_of[16], (D, QKV), jnp.float32) ** shard_levels(streams_of[16], (D, QKV), ((0, 8),), -0.2, 0.2)), 1.7537952427121306e-12, 7.0151809708485224e-12)
    attend_out_second = jnp.clip(jnp.exp(math.log(7.0151809708485224e-12) - 1.3862944 * jax.random.uniform(streams_of[17], (D, D), jnp.float32) ** shard_levels(streams_of[17], (D, D), ((0, 8),), -0.2, 0.2)), 1.7537952427121306e-12, 7.0151809708485224e-12)
    feed_in_second = jnp.clip(jnp.exp(math.log(7.0151809708485224e-12) - 1.3862944 * jax.random.uniform(streams_of[18], (D, 2 * FF), jnp.float32) ** shard_levels(streams_of[18], (D, 2 * FF), ((0, 8),), -0.2, 0.2)), 1.7537952427121306e-12, 7.0151809708485224e-12)
    feed_out_second = jnp.clip(jnp.exp(math.log(7.0151809708485224e-12) - 1.3862944 * jax.random.uniform(streams_of[19], (FF, D), jnp.float32) ** shard_levels(streams_of[19], (FF, D), ((0, 8),), -0.2, 0.2)), 1.7537952427121306e-12, 7.0151809708485224e-12)
    norm_gains_second = jnp.clip(jnp.exp(math.log(7.0151809708485224e-12) - 1.3862944 * jax.random.uniform(streams_of[20], (3, D), jnp.float32) ** shard_levels(streams_of[20], (3, D), ((1, 8),), -0.2, 0.2)), 1.7537952427121306e-12, 7.0151809708485224e-12)
    embed_table_second = jnp.clip(jnp.exp(math.log(7.0151809708485224e-12) - 1.3862944 * jax.random.uniform(streams_of[21], (VOCAB, D), jnp.float32) ** shard_levels(streams_of[21], (VOCAB, D), ((0, 32),), -0.2, 0.2)), 1.7537952427121306e-12, 7.0151809708485224e-12)
    return {"token_ids": token_ids, "seq_lengths": seq_lengths, "completion_mask": completion_mask, "deal": deal, "attend_in": attend_in, "attend_out": attend_out, "feed_in": feed_in, "feed_out": feed_out, "norm_gains": norm_gains, "embed_table": embed_table, "attend_in_first": attend_in_first, "attend_out_first": attend_out_first, "feed_in_first": feed_in_first, "feed_out_first": feed_out_first, "norm_gains_first": norm_gains_first, "embed_table_first": embed_table_first, "attend_in_second": attend_in_second, "attend_out_second": attend_out_second, "feed_in_second": feed_in_second, "feed_out_second": feed_out_second, "norm_gains_second": norm_gains_second, "embed_table_second": embed_table_second}


@jax.custom_vjp
def low(v):
    return lax.optimization_barrier(v.astype(jnp.bfloat16)).astype(jnp.float32)

@jax.custom_vjp
def low_back(v):
    return v

def low_keep(v):
    return (low(v), None)

def low_pass(kept, grad):
    return (grad,)

def back_keep(v):
    return (v, None)

def back_low(kept, grad):
    return (low(grad),)
low.defvjp(low_keep, low_pass)
low_back.defvjp(back_keep, back_low)
eps_norm = 1e-05
rope_base = 100000.0
beta_one = 0.5
beta_two = 0.5
adam_eps = 1e-08
learn_rate = 0.008
weight_decay = 0.1
max_norm = 0.01
highest = lax.Precision.HIGHEST

def rms_norm(rows_in, gain_row):
    scale_rows = lax.rsqrt(lax.optimization_barrier(jnp.mean(rows_in * rows_in, axis=-1, keepdims=True)) + eps_norm)
    return rows_in * scale_rows * gain_row

def rotation(positions):
    half_dim = HEAD_DIM // 2
    freqs = rope_base ** (-jnp.arange(half_dim).astype(jnp.float32) * 2.0 / HEAD_DIM)
    angles = positions[:, None] * freqs[None, :]
    return (jnp.cos(angles)[:, None, :], jnp.sin(angles)[:, None, :])

def rotate(rows_in, cos_rows, sin_rows):
    half_dim = rows_in.shape[-1] // 2
    first_half = rows_in[..., :half_dim]
    second_half = rows_in[..., half_dim:]
    return jnp.concatenate([first_half * cos_rows - second_half * sin_rows, second_half * cos_rows + first_half * sin_rows], axis=-1)

def vocab_pass(picked, embed_table, targets):
    vocab_block = math.gcd(VOCAB // 2, 4096)
    block_count = VOCAB // vocab_block
    blocks = embed_table.reshape(block_count, vocab_block, D)
    starts = (jnp.arange(block_count, dtype=jnp.int32) * jnp.int32(vocab_block)).astype(jnp.int32)

    def block_logits(block_rows):
        return low_back(jnp.dot(picked, block_rows.T, precision=highest))

    def block_hits(logits, block_start):
        column_ids = (block_start + jnp.arange(vocab_block, dtype=jnp.int32)).astype(jnp.int32)
        return lax.optimization_barrier(jnp.sum(jnp.where(column_ids[None, :] == targets[:, None], logits, 0.0), axis=1))
    first_logits = block_logits(blocks[0])
    first_top = lax.optimization_barrier(jnp.max(first_logits, axis=1))
    first_total = lax.optimization_barrier(jnp.sum(jnp.exp(first_logits - first_top[:, None]), axis=1))
    first_hits = block_hits(first_logits, starts[0])

    def step_block(running, block_pack):
        row_top, row_total, hit_sum = running
        block_rows, block_start = block_pack
        logits = block_logits(block_rows)
        new_top = jnp.maximum(row_top, lax.optimization_barrier(jnp.max(logits, axis=1)))
        row_total = row_total * jnp.exp(row_top - new_top) + lax.optimization_barrier(jnp.sum(jnp.exp(logits - new_top[:, None]), axis=1))
        hit_sum = hit_sum + block_hits(logits, block_start)
        return ((new_top, row_total, hit_sum), None)
    (row_top, row_total, hit_sum), _ = lax.scan(jax.checkpoint(step_block), (first_top, first_total, first_hits), (blocks[1:], starts[1:]))
    return (row_top + jnp.log(row_total), hit_sum)

def pack_buffers(token_ids, completion_mask, seq_lengths, deal):
    seq_numbers = jnp.arange(SEQS, dtype=jnp.int32)
    places = (seq_numbers // GROUP_SEQS * GROUP_SEQS + deal.astype(jnp.int32)).astype(jnp.int32)
    sources = jnp.zeros((SEQS,), jnp.int32).at[places].set(seq_numbers)
    pairs = sources.reshape(SEQS // 2, 2)
    first_len = jnp.take(seq_lengths.astype(jnp.int32), pairs[:, 0]).astype(jnp.int32)
    step_ids = jnp.arange(SLOT, dtype=jnp.int32)
    index_rows = jnp.clip(SLOT - first_len[:, None] + step_ids[None, :], 0, SLOT - 1).astype(jnp.int32)
    in_front = step_ids[None, :] < first_len[:, None]

    def pack_one(table):
        front = jnp.take_along_axis(jnp.take(table, pairs[:, 0], axis=0), index_rows, axis=1)
        back = jnp.take(table, pairs[:, 1], axis=0)
        return jnp.where(in_front, front, back).astype(jnp.int32)
    return (pack_one(token_ids.astype(jnp.int32)), pack_one(completion_mask.astype(jnp.int32)), first_len, places)

def slot_loss(weights, slot_ids, first_len, slot_mask):
    attend_in, attend_out, feed_in, feed_out, norm_gains, embed_table = weights
    step_ids = jnp.arange(SLOT, dtype=jnp.int32)
    segment = (step_ids >= first_len).astype(jnp.int32)
    positions = (step_ids - segment * first_len).astype(jnp.float32)
    cos_rows, sin_rows = rotation(positions)
    group_size = HEADS // KV_HEADS
    embedded = low_back(jnp.take(embed_table, slot_ids, axis=0))
    normed_one = low(rms_norm(embedded, norm_gains[0]))
    mixed_rows = low_back(jnp.dot(normed_one, attend_in, precision=highest))
    queries = low(rotate(mixed_rows[:, :D].reshape(SLOT, HEADS, HEAD_DIM), cos_rows, sin_rows))
    key_rows = low(rotate(mixed_rows[:, D:D + KVD].reshape(SLOT, KV_HEADS, HEAD_DIM), cos_rows, sin_rows))
    value_rows = low(mixed_rows[:, D + KVD:].reshape(SLOT, KV_HEADS, HEAD_DIM))
    key_wide = jnp.repeat(key_rows, group_size, axis=1)
    value_wide = jnp.repeat(value_rows, group_size, axis=1)
    scores = low_back(jnp.einsum('qhd,khd->hqk', queries, key_wide, precision=highest) * 0.125)
    allowed = ((step_ids[None, :] <= step_ids[:, None]) & (segment[None, :] == segment[:, None]))[None]
    safe_scores = jnp.where(allowed, scores, 0.0)
    row_top = lax.optimization_barrier(jnp.max(jnp.where(allowed, safe_scores, -10000.0), axis=-1, keepdims=True))
    exp_rows = jnp.where(allowed, jnp.exp(safe_scores - row_top), 0.0)
    prob_rows = low(exp_rows / lax.optimization_barrier(jnp.sum(exp_rows, axis=-1, keepdims=True)))
    attended = low(low_back(jnp.einsum('hqk,khd->qhd', prob_rows, value_wide, precision=highest))).reshape(SLOT, D)
    resid_one = embedded + low_back(jnp.dot(attended, attend_out, precision=highest))
    normed_two = low(rms_norm(resid_one, norm_gains[1]))
    gate_up = low_back(jnp.dot(normed_two, feed_in, precision=highest))
    hidden = low(low_back(jax.nn.silu(gate_up[:, :FF]) * gate_up[:, FF:]))
    resid_two = resid_one + low_back(jnp.dot(hidden, feed_out, precision=highest))
    final_rows = low(rms_norm(resid_two, norm_gains[2]))
    chosen = jnp.nonzero(slot_mask, size=2 * COMP)[0].astype(jnp.int32)
    picked = jnp.take(final_rows, chosen, axis=0)
    targets = jnp.take(slot_ids, (chosen + 1).astype(jnp.int32)).astype(jnp.int32)
    lse_rows, target_logit = vocab_pass(picked, embed_table, targets)
    return lse_rows - target_logit

def adamw_update(master, first_old, second_old, gradient, decay_on):
    first_new = beta_one * first_old + (1.0 - beta_one) * gradient
    second_new = beta_two * second_old + (1.0 - beta_two) * gradient * gradient
    first_hat = first_new / (1.0 - beta_one ** STEP)
    second_hat = second_new / (1.0 - beta_two ** STEP)
    change = -learn_rate * (first_hat / (jnp.sqrt(second_hat) + adam_eps) + decay_on * weight_decay * master)
    return (master + change, first_new, second_new, change)

def reference(token_ids, seq_lengths, completion_mask, deal, attend_in, attend_out, feed_in, feed_out, norm_gains, embed_table, attend_in_first, attend_out_first, feed_in_first, feed_out_first, norm_gains_first, embed_table_first, attend_in_second, attend_out_second, feed_in_second, feed_out_second, norm_gains_second, embed_table_second):
    masters = (attend_in, attend_out, feed_in, feed_out, norm_gains, embed_table)
    firsts = (attend_in_first, attend_out_first, feed_in_first, feed_out_first, norm_gains_first, embed_table_first)
    seconds = (attend_in_second, attend_out_second, feed_in_second, feed_out_second, norm_gains_second, embed_table_second)
    buf_ids, buf_masks, first_lens, places = pack_buffers(token_ids, completion_mask, seq_lengths, deal)

    def total_loss(weights):
        rounded = tuple((low(weight) for weight in weights))

        def one_slot(running, slot_pack):
            row_losses = slot_loss(rounded, slot_pack[0], slot_pack[1], slot_pack[2])
            return (running + jnp.sum(row_losses), row_losses)
        start_sum = jnp.zeros((), jnp.float32)
        loss_sum, all_rows = lax.scan(jax.checkpoint(one_slot), start_sum, (buf_ids, first_lens, buf_masks))
        return (loss_sum / COUNT, all_rows)
    mean_loss, pull_back, all_rows = jax.vjp(total_loss, masters, has_aux=True)
    gradients = pull_back(jnp.ones_like(mean_loss))[0]
    packed_loss = lax.optimization_barrier(jnp.mean(all_rows.reshape(SEQS, COMP), axis=1))
    seq_loss = jnp.take(packed_loss, places)
    squares = sum((jnp.sum(gradient * gradient) for gradient in gradients))
    grad_norm = jnp.sqrt(squares)
    factor = max_norm / jnp.maximum(grad_norm, max_norm)
    decays = (1.0, 1.0, 1.0, 1.0, 0.0, 1.0)
    updated = [adamw_update(masters[number], firsts[number], seconds[number], gradients[number] * factor, decays[number]) for number in range(6)]
    return (updated[0][0], updated[1][0], updated[2][0], updated[3][0], updated[4][3], updated[5][0], updated[0][1], updated[1][1], updated[2][1], updated[3][1], updated[4][1], updated[5][1], updated[0][2], updated[1][2], updated[2][2], updated[3][2], updated[4][2], updated[5][2], mean_loss, grad_norm, seq_loss)
```

```python
import functools

import jax
import jax.numpy as jnp
import numpy as np
from jax import lax
from jax.experimental import pallas as pl
from jax.experimental.pallas import tpu as pltpu
from jax.sharding import PartitionSpec as P

MESH = pl.DeviceIdType.MESH
VMEM = pltpu.MemorySpace.VMEM

HEADS = 15
KV_HEADS = 5
HEAD_DIM = 64
COMP = 16
STEP = 3


eps_norm = 1e-05
rope_base = 100000.0
beta_one = 0.5
beta_two = 0.5
adam_eps = 1e-08
learn_rate = 0.008
weight_decay = 0.1
max_norm = 0.01
masked_score = -1e30


def bits_of(size):
    return [1 << bit for bit in reversed(range(size.bit_length() - 1))]


def place_of(dp_at, shard_at, dp_size, shard_size):
    place, weight = 0, 1
    for index, size in ((dp_at, dp_size), (shard_at, shard_size)):
        for bit in bits_of(size):
            place = place + (index // bit) % 2 * weight
            weight *= 2
    return place


def exchange_stages(dp_size, shard_size):
    return [(0, bit) for bit in bits_of(dp_size)] + [(1, bit) for bit in bits_of(shard_size)]


def partner_of(me, axis, bit):
    other = list(me)
    other[axis] = me[axis] + bit - 2 * bit * ((me[axis] // bit) % 2)
    return tuple(other)


def here():
    return (lax.axis_index("dp"), lax.axis_index("shard"))


def greet_partners(me, stages):
    barrier = pltpu.get_barrier_semaphore()
    for axis, bit in stages:
        pl.semaphore_signal(
            barrier, inc=1, device_id=partner_of(me, axis, bit), device_id_type=MESH
        )
    pl.semaphore_wait(barrier, len(stages))


def gather_kernel(sizes, x_ref, out_ref, send_sem, recv_sem, own_sem):
    me = here()
    stages = exchange_stages(*sizes)
    place = place_of(*me, *sizes)
    greet_partners(me, stages)
    own = pltpu.make_async_copy(x_ref, out_ref.at[place], own_sem)
    own.start()
    own.wait()
    for number, (axis, bit) in enumerate(stages):
        span = 1 << number
        start = place // span * span
        copy = pltpu.make_async_remote_copy(
            src_ref=out_ref.at[pl.ds(start, span)],
            dst_ref=out_ref.at[pl.ds(start, span)],
            send_sem=send_sem.at[number],
            recv_sem=recv_sem.at[number],
            device_id=partner_of(me, axis, bit),
            device_id_type=MESH,
        )
        copy.start()
        copy.wait()


def gather_all(block, sizes, collective_id, name):
    total = sizes[0] * sizes[1]
    count = len(exchange_stages(*sizes))
    return pl.pallas_call(
        functools.partial(gather_kernel, sizes),
        name=name,
        out_shape=jax.ShapeDtypeStruct((total,) + block.shape, block.dtype),
        in_specs=[pl.BlockSpec(memory_space=VMEM)],
        out_specs=pl.BlockSpec(memory_space=VMEM),
        scratch_shapes=[
            pltpu.SemaphoreType.DMA((count,)),
            pltpu.SemaphoreType.DMA((count,)),
            pltpu.SemaphoreType.DMA,
        ],
        compiler_params=pltpu.CompilerParams(collective_id=collective_id, has_side_effects=True),
    )(block)


def scatter_kernel(sizes, x_ref, out_ref, total_ref, landed, send_sem, recv_sem):
    me = here()
    stages = exchange_stages(*sizes)
    place = place_of(*me, *sizes)
    greet_partners(me, stages)
    base = 0
    first = len(stages) - 1
    for number in reversed(range(len(stages))):
        axis, bit = stages[number]
        span = 1 << number
        mine = place // span * span
        other = mine + span - 2 * span * ((mine // span) % 2)
        parent = place // (2 * span) * (2 * span)
        slot = landed.at[pl.ds(base, span)]
        source = x_ref if number == first else total_ref
        shift = 0 if number == first else parent
        copy = pltpu.make_async_remote_copy(
            src_ref=source.at[pl.ds(other - shift, span)],
            dst_ref=slot,
            send_sem=send_sem.at[number],
            recv_sem=recv_sem.at[number],
            device_id=partner_of(me, axis, bit),
            device_id_type=MESH,
        )
        copy.start()
        copy.wait()
        kept = source[pl.ds(mine - shift, span)]
        if number:
            total_ref[pl.ds(0, span)] = kept + landed[base : base + span]
        else:
            out_ref[...] = (kept + landed[base : base + span])[0]
        base += span


def scatter_all(blocks, sizes, collective_id, name):
    total = sizes[0] * sizes[1]
    count = len(exchange_stages(*sizes))
    return pl.pallas_call(
        functools.partial(scatter_kernel, sizes),
        name=name,
        out_shape=jax.ShapeDtypeStruct(blocks.shape[1:], blocks.dtype),
        in_specs=[pl.BlockSpec(memory_space=VMEM)],
        out_specs=pl.BlockSpec(memory_space=VMEM),
        scratch_shapes=[
            pltpu.VMEM((total // 2,) + blocks.shape[1:], blocks.dtype),
            pltpu.VMEM((total,) + blocks.shape[1:], blocks.dtype),
            pltpu.SemaphoreType.DMA((count,)),
            pltpu.SemaphoreType.DMA((count,)),
        ],
        compiler_params=pltpu.CompilerParams(collective_id=collective_id, has_side_effects=True),
    )(blocks)


def deal_kernel(
    sizes, rows_ref, note_ref, out_ref, notes_ref, send_sem, recv_sem, note_send, note_recv, own_sem
):
    total = sizes[0] * sizes[1]
    dp_at, shard_at = here()
    me = dp_at * sizes[1] + shard_at
    barrier = pltpu.get_barrier_semaphore()

    def peer_at(step):
        peer = lax.rem(me + step, total)
        return peer, (peer // sizes[1], peer % sizes[1])

    @pl.loop(1, total)
    def _(step):
        pl.semaphore_signal(barrier, inc=1, device_id=peer_at(step)[1], device_id_type=MESH)

    own = pltpu.make_async_copy(rows_ref.at[me], out_ref.at[me], own_sem.at[0])
    own.start()
    own_note = pltpu.make_async_copy(note_ref, notes_ref.at[me], own_sem.at[1])
    own_note.start()
    pl.semaphore_wait(barrier, total - 1)

    def copies(step):
        peer, device = peer_at(step)
        return (
            pltpu.make_async_remote_copy(
                src_ref=note_ref,
                dst_ref=notes_ref.at[me],
                send_sem=note_send.at[peer],
                recv_sem=note_recv.at[me],
                device_id=device,
                device_id_type=MESH,
            ),
            pltpu.make_async_remote_copy(
                src_ref=rows_ref.at[peer],
                dst_ref=out_ref.at[me],
                send_sem=send_sem.at[peer],
                recv_sem=recv_sem.at[me],
                device_id=device,
                device_id_type=MESH,
            ),
        )

    @pl.loop(1, total)
    def _(step):
        for copy in copies(step):
            copy.start()

    own.wait()
    own_note.wait()

    @pl.loop(1, total)
    def _(step):
        peer, device = peer_at(step)
        for copy in copies(step):
            copy.wait_send()
        pltpu.make_async_remote_copy(
            src_ref=note_ref,
            dst_ref=notes_ref.at[peer],
            send_sem=note_send.at[peer],
            recv_sem=note_recv.at[peer],
            device_id=device,
            device_id_type=MESH,
        ).wait_recv()
        pltpu.make_async_remote_copy(
            src_ref=rows_ref.at[peer],
            dst_ref=out_ref.at[peer],
            send_sem=send_sem.at[peer],
            recv_sem=recv_sem.at[peer],
            device_id=device,
            device_id_type=MESH,
        ).wait_recv()


def deal_rows(rows, note, sizes, collective_id, name):
    total = sizes[0] * sizes[1]
    return pl.pallas_call(
        functools.partial(deal_kernel, sizes),
        name=name,
        out_shape=(
            jax.ShapeDtypeStruct(rows.shape, rows.dtype),
            jax.ShapeDtypeStruct((total,) + note.shape, note.dtype),
        ),
        in_specs=[pl.BlockSpec(memory_space=VMEM)] * 2,
        out_specs=(pl.BlockSpec(memory_space=VMEM),) * 2,
        scratch_shapes=[pltpu.SemaphoreType.DMA((total,))] * 4 + [pltpu.SemaphoreType.DMA((2,))],
        compiler_params=pltpu.CompilerParams(collective_id=collective_id, has_side_effects=True),
    )(rows, note)


def count_kernel(high_count, high_ref, low_ref, out_ref):
    high_pad = out_ref.shape[1]

    @pl.loop(0, high_ref.shape[0])
    def _(n):
        length = high_ref.shape[2]
        high_hot = (
            lax.broadcasted_iota(jnp.int32, (high_pad, length), 0) == high_ref[n]
        ).astype(jnp.float32)
        low_hot = (lax.broadcasted_iota(jnp.int32, (128, length), 0) == low_ref[n]).astype(
            jnp.float32
        )
        out_ref[n] = contract_last(high_hot.astype(jnp.bfloat16), low_hot.astype(jnp.bfloat16))


def count_rows(high, low, high_pad):
    count, length = high.shape
    return pl.pallas_call(
        functools.partial(count_kernel, high_pad),
        name="count_rows",
        out_shape=jax.ShapeDtypeStruct((count, high_pad, 128), jnp.float32),
        in_specs=[pl.BlockSpec(memory_space=VMEM)] * 2,
        out_specs=pl.BlockSpec(memory_space=VMEM),
    )(high.reshape(count, 1, length), low.reshape(count, 1, length))


def contract_last(left, right):
    return lax.dot_general(
        left, right, (((1,), (1,)), ((), ())), preferred_element_type=jnp.float32
    )


def contract_first(left, right):
    return lax.dot_general(
        left, right, (((0,), (0,)), ((), ())), preferred_element_type=jnp.float32
    )


def rms_scale(rows_in):
    return lax.rsqrt(jnp.mean(rows_in * rows_in, axis=-1, keepdims=True) + eps_norm)


def norm_back(rows_in, gain_row, incoming):
    scale_rows = rms_scale(rows_in)
    weighted = incoming * gain_row
    d_rows = scale_rows * weighted - rows_in * (scale_rows * scale_rows * scale_rows) * jnp.mean(
        weighted * rows_in, axis=-1, keepdims=True
    )
    return (d_rows, jnp.sum(incoming * rows_in * scale_rows, axis=0))


def rotation(positions):
    half_dim = HEAD_DIM // 2
    freqs = rope_base ** (-jnp.arange(half_dim, dtype=jnp.float32) * 2.0 / HEAD_DIM)
    angles = positions[:, None] * freqs[None, :]
    return (jnp.cos(angles)[:, None, :], jnp.sin(angles)[:, None, :])


def rotate(rows_in, cos_rows, sin_rows, turn_sign):
    half_dim = rows_in.shape[-1] // 2
    first_half = rows_in[..., :half_dim]
    second_half = rows_in[..., half_dim:]
    return jnp.concatenate(
        [
            first_half * cos_rows - turn_sign * second_half * sin_rows,
            second_half * cos_rows + turn_sign * first_half * sin_rows,
        ],
        axis=-1,
    )


def adamw_update(master, first_old, second_old, gradient, decay_on):
    first_new = beta_one * first_old + (1.0 - beta_one) * gradient
    second_new = beta_two * second_old + (1.0 - beta_two) * gradient * gradient
    first_hat = first_new / (1.0 - beta_one**STEP)
    second_hat = second_new / (1.0 - beta_two**STEP)
    change = -learn_rate * (
        first_hat / (jnp.sqrt(second_hat) + adam_eps) + decay_on * weight_decay * master
    )
    return (master + change, first_new, second_new, change)


def per_device(
    token_ids,
    seq_lengths,
    completion_mask,
    deal,
    attend_in,
    attend_out,
    feed_in,
    feed_out,
    norm_gains,
    embed_table,
    attend_in_first,
    attend_out_first,
    feed_in_first,
    feed_out_first,
    norm_gains_first,
    embed_table_first,
    attend_in_second,
    attend_out_second,
    feed_in_second,
    feed_out_second,
    norm_gains_second,
    embed_table_second,
):
    shard_count = lax.axis_size("shard")
    group_count = lax.axis_size("dp")
    sizes = (group_count, shard_count)
    device_count = shard_count * group_count
    dp_me, shard_me = here()
    device_me = dp_me * shard_count + shard_me
    place_me = place_of(dp_me, shard_me, *sizes)
    total_rows = 2 * COMP * device_count
    slot_len = token_ids.shape[1]
    model_width = attend_out.shape[1]
    masters = (attend_in, attend_out, feed_in, feed_out, norm_gains)
    copies = tuple((master.astype(jnp.bfloat16) for master in masters))
    w_qkv, w_out, w_gate_up, w_down, gain_rows = (
        lax.all_gather(copies[0], "shard", axis=0, tiled=True),
        lax.all_gather(copies[1], "shard", axis=0, tiled=True),
        lax.all_gather(copies[2], "shard", axis=0, tiled=True),
        lax.all_gather(copies[3], "shard", axis=0, tiled=True),
        lax.all_gather(copies[4], "shard", axis=1, tiled=True),
    )
    table_rows = embed_table.astype(jnp.bfloat16)
    rows_dev = embed_table.shape[0]
    gains_full = gain_rows.astype(jnp.float32)
    kv_width = KV_HEADS * HEAD_DIM
    ff_width = w_down.shape[0]
    group_size = HEADS // KV_HEADS
    row_count = 2 * COMP

    side = jnp.concatenate(
        [
            seq_lengths[:, None],
            deal[:, None],
            jnp.zeros((token_ids.shape[0], 126), jnp.int32),
        ],
        axis=1,
    )
    seqs_all = gather_all(
        jnp.concatenate([token_ids * 2 + completion_mask, side], axis=1), sizes, 1, "gather_ids"
    )
    seqs_all = seqs_all.reshape(-1, slot_len + 128)
    lengths_all = seqs_all[:, slot_len]
    places_all = seqs_all[:, slot_len + 1]
    order = sorted(
        ((dp_at, shard_at) for dp_at in range(group_count) for shard_at in range(shard_count)),
        key=lambda at: place_of(*at, *sizes),
    )
    seqs_dev = token_ids.shape[0]
    group_of = jnp.asarray(np.repeat([at[0] for at in order], seqs_dev).astype(np.int32))
    buffer_of = group_of * shard_count + places_all // 2
    step_ids = jnp.arange(slot_len, dtype=jnp.int32)

    def own_row(half):
        hit = (group_of == dp_me) & (places_all == 2 * shard_me + half)
        return jnp.sum(jnp.where(hit[:, None], seqs_all, 0), axis=0)

    front_row, back_row = own_row(0), own_row(1)
    first_len = front_row[slot_len]
    front_slot = front_row[:slot_len]
    packed = jnp.where(
        step_ids < first_len,
        lax.dynamic_slice_in_dim(
            jnp.concatenate([front_slot, front_slot]), slot_len - first_len, slot_len
        ),
        back_row[:slot_len],
    )
    own_ids = packed // 2
    own_marks = packed % 2
    marks_before = jnp.sum(
        jnp.where(step_ids[None, :] <= step_ids[:, None], own_marks[None, :], 0), axis=1
    )
    chosen_hot = (
        marks_before[None, :] == 1 + jnp.arange(row_count, dtype=jnp.int32)[:, None]
    ) & (own_marks[None, :] == 1)
    own_targets = jnp.sum(jnp.where(chosen_hot, jnp.roll(own_ids, -1)[None, :], 0), axis=1)
    segment = (step_ids >= first_len).astype(jnp.int32)
    cos_rows, sin_rows = rotation((step_ids - segment * first_len).astype(jnp.float32))

    deal_cap = -(-3 * slot_len // (2 * device_count) // 16) * 16
    ids_all = seqs_all[:, :slot_len] // 2
    near = ids_all - device_me * rows_dev
    wanted = (
        (near >= 0)
        & (near < rows_dev)
        & (step_ids[None, :] >= slot_len - lengths_all[:, None])
    )
    high_count = -(-rows_dev // 128)
    high_pad = -(-high_count // 8) * 8
    seen = count_rows(
        jnp.where(wanted, near // 128, -1), jnp.where(wanted, near % 128, -1), high_pad
    )[:, :high_count]
    buffer_hot = (
        buffer_of[None, :] == jnp.arange(device_count, dtype=jnp.int32)[:, None]
    ).astype(jnp.float32)
    seen_by = (
        jnp.einsum("bn,nhl->bhl", buffer_hot, jnp.minimum(seen, 1.0)) > 0.5
    ).astype(jnp.float32)
    upto = (jnp.arange(128)[:, None] <= jnp.arange(128)[None, :]).astype(jnp.float32)
    within = jnp.einsum("bhl,lm->bhm", seen_by, upto)
    whole = within[:, :, -1]
    before = (jnp.arange(high_count)[:, None] < jnp.arange(high_count)[None, :]).astype(jnp.float32)
    rank_by = within + jnp.einsum("bh,hg->bg", whole, before)[:, :, None]
    rank_by = jnp.where(seen_by > 0.5, rank_by, 0.0).reshape(device_count, -1)[:, :rows_dev]

    owner = own_ids // rows_dev
    same_id = own_ids[None, :] == own_ids[:, None]
    is_first = (
        jnp.sum(jnp.where(same_id & (step_ids[None, :] < step_ids[:, None]), 1, 0), axis=1) == 0
    )
    rank_own = jnp.sum(
        jnp.where(
            is_first[None, :]
            & (owner[None, :] == owner[:, None])
            & (own_ids[None, :] < own_ids[:, None]),
            1,
            0,
        ),
        axis=1,
    )
    rounds_own = jnp.max(rank_own) // deal_cap + 1

    def send_hot(turn):
        spots = (turn * deal_cap + 1 + jnp.arange(deal_cap, dtype=jnp.int32)).astype(jnp.float32)
        return (
            (rank_by[:, None, :] == spots[None, :, None])
            .astype(jnp.bfloat16)
            .reshape(device_count * deal_cap, rows_dev)
        )

    def take_hot(turn):
        slot = rank_own - turn * deal_cap
        inside = (slot >= 0) & (slot < deal_cap)
        spot = jnp.where(inside, owner * deal_cap + slot, -1)
        return (
            spot[:, None] == jnp.arange(device_count * deal_cap, dtype=jnp.int32)[None, :]
        ).astype(jnp.bfloat16)

    def fetch(turn, note):
        rows_out = jnp.dot(send_hot(turn), table_rows, preferred_element_type=jnp.float32)
        landed, notes = deal_rows(
            rows_out.astype(jnp.bfloat16).reshape(device_count, deal_cap, model_width),
            note,
            sizes,
            2,
            "deal_rows",
        )
        found = jnp.dot(
            take_hot(turn),
            landed.reshape(device_count * deal_cap, model_width),
            preferred_element_type=jnp.float32,
        )
        return found, notes

    note_shape = (-(-3 * model_width // 1024) * 8, 128)
    embedded, round_notes = fetch(
        0, jnp.broadcast_to(rounds_own.astype(jnp.float32), note_shape)
    )
    rounds = jnp.max(round_notes[:, 0, 0]).astype(jnp.int32)
    embedded = lax.fori_loop(
        1,
        rounds,
        lambda turn, held: held + fetch(turn, jnp.zeros(note_shape, jnp.float32))[0],
        embedded,
    )
    normed_one = (embedded * rms_scale(embedded) * gains_full[0]).astype(jnp.bfloat16)
    mixed_rows = jnp.dot(normed_one, w_qkv, preferred_element_type=jnp.float32)
    queries = rotate(
        mixed_rows[:, :model_width].reshape(slot_len, HEADS, HEAD_DIM), cos_rows, sin_rows, 1.0
    ).astype(jnp.bfloat16)
    key_rows = rotate(
        mixed_rows[:, model_width : model_width + kv_width].reshape(slot_len, KV_HEADS, HEAD_DIM),
        cos_rows,
        sin_rows,
        1.0,
    ).astype(jnp.bfloat16)
    value_rows = (
        mixed_rows[:, model_width + kv_width :]
        .reshape(slot_len, KV_HEADS, HEAD_DIM)
        .astype(jnp.bfloat16)
    )
    key_wide = jnp.repeat(key_rows, group_size, axis=1)
    value_wide = jnp.repeat(value_rows, group_size, axis=1)
    block_len = min(512, slot_len)

    def block_scores(first_row):
        query_block = queries[first_row : first_row + block_len]
        raw_scores = (
            jnp.einsum("qhd,khd->hqk", query_block, key_wide, preferred_element_type=jnp.float32)
            * 0.125
        )
        rows_here = step_ids[first_row : first_row + block_len]
        segment_here = segment[first_row : first_row + block_len]
        allowed = (step_ids[None, :] <= rows_here[:, None]) & (
            segment[None, :] == segment_here[:, None]
        )
        return (query_block, jnp.where(allowed[None], raw_scores, masked_score))

    block_outputs = []
    lse_blocks = []
    for first_row in range(0, slot_len, block_len):
        _, scores = block_scores(first_row)
        row_top = jnp.max(scores, axis=-1, keepdims=True)
        exp_rows = jnp.exp(scores - row_top)
        row_total = jnp.sum(exp_rows, axis=-1, keepdims=True)
        prob_rows = (exp_rows / row_total).astype(jnp.bfloat16)
        block_outputs.append(
            jnp.einsum(
                "hqk,khd->qhd", prob_rows, value_wide, preferred_element_type=jnp.float32
            ).astype(jnp.bfloat16)
        )
        lse_blocks.append(row_top + jnp.log(row_total))
    attended = jnp.concatenate(block_outputs, axis=0).reshape(slot_len, model_width)
    resid_one = embedded + jnp.dot(attended, w_out, preferred_element_type=jnp.float32)
    normed_two = (resid_one * rms_scale(resid_one) * gains_full[1]).astype(jnp.bfloat16)
    gate_up = jnp.dot(normed_two, w_gate_up, preferred_element_type=jnp.float32)
    gate_part = gate_up[:, :ff_width]
    up_part = gate_up[:, ff_width:]
    hidden = (jax.nn.silu(gate_part) * up_part).astype(jnp.bfloat16)
    resid_two = resid_one + jnp.dot(hidden, w_down, preferred_element_type=jnp.float32)
    final_rows = (resid_two * rms_scale(resid_two) * gains_full[2]).astype(jnp.bfloat16)
    chosen_rows = chosen_hot.astype(jnp.bfloat16)
    picked = jnp.dot(chosen_rows, final_rows, preferred_element_type=jnp.float32)
    pad_width = -(-(model_width + 2) // 128) * 128 - model_width - 2
    tagged = jnp.concatenate(
        [
            picked,
            (own_targets // 256).astype(jnp.float32)[:, None],
            (own_targets % 256).astype(jnp.float32)[:, None],
            jnp.zeros((row_count, pad_width), jnp.float32),
        ],
        axis=1,
    ).astype(jnp.bfloat16)
    tagged_all = gather_all(tagged, sizes, 3, "gather_rows").reshape(total_rows, -1)
    rows_all = tagged_all[:, :model_width]
    targets_all = tagged_all[:, model_width].astype(jnp.int32) * 256 + tagged_all[
        :, model_width + 1
    ].astype(jnp.int32)
    logits = contract_last(rows_all, table_rows)
    target_hot = (targets_all - device_me * rows_dev)[:, None] == jnp.arange(
        rows_dev, dtype=jnp.int32
    )[None, :]
    top_logit = jnp.max(logits, axis=1)
    sum_exp = jnp.sum(jnp.exp(logits - top_logit[:, None]), axis=1)
    target_logit = jnp.sum(jnp.where(target_hot, logits, 0.0), axis=1)
    stats = gather_all(
        jnp.concatenate([top_logit, sum_exp, target_logit]).reshape(3 * total_rows // 128, 128),
        sizes,
        4,
        "gather_stats",
    ).reshape(device_count, 3, total_rows)
    top_all = jnp.max(stats[:, 0], axis=0)
    sum_all = jnp.sum(stats[:, 1] * jnp.exp(stats[:, 0] - top_all[None, :]), axis=0)
    lse_vocab = top_all + jnp.log(sum_all)
    row_losses = lse_vocab - jnp.sum(stats[:, 2], axis=0)
    mean_loss = jnp.sum(row_losses) / total_rows
    packed_loss = jnp.mean(row_losses.reshape(-1, COMP), axis=1)
    loss_at = place_of(dp_me, deal // 2, *sizes) * 2 + deal % 2
    seq_loss = jnp.sum(
        jnp.where(
            loss_at[:, None] == jnp.arange(packed_loss.shape[0], dtype=jnp.int32)[None, :],
            packed_loss[None, :],
            0.0,
        ),
        axis=1,
    )
    d_logits = (
        (jnp.exp(logits - lse_vocab[:, None]) - target_hot.astype(jnp.float32)) / total_rows
    ).astype(jnp.bfloat16)
    d_table_head = contract_first(d_logits, rows_all)
    d_picked = scatter_all(
        jnp.dot(d_logits, table_rows, preferred_element_type=jnp.float32).reshape(
            device_count, row_count, model_width
        ),
        sizes,
        5,
        "scatter_rows",
    )
    d_final = lax.dot_general(
        chosen_hot.astype(jnp.float32),
        d_picked,
        (((0,), (0,)), ((), ())),
        precision=lax.Precision.HIGHEST,
        preferred_element_type=jnp.float32,
    )
    d_resid_two, d_gain_three = norm_back(resid_two, gains_full[2], d_final)
    d_down = d_resid_two.astype(jnp.bfloat16)
    grad_down = contract_first(hidden, d_down)
    d_hidden = contract_last(d_down, w_down).astype(jnp.bfloat16).astype(jnp.float32)
    gate_sigmoid = jax.nn.sigmoid(gate_part)
    d_gate = d_hidden * up_part * gate_sigmoid * (1.0 + gate_part * (1.0 - gate_sigmoid))
    d_up = d_hidden * jax.nn.silu(gate_part)
    d_gate_up = jnp.concatenate([d_gate, d_up], axis=1).astype(jnp.bfloat16)
    grad_gate_up = contract_first(normed_two, d_gate_up)
    d_normed_two = contract_last(d_gate_up, w_gate_up)
    d_resid_norm, d_gain_two = norm_back(resid_one, gains_full[1], d_normed_two)
    d_resid_one = d_resid_two + d_resid_norm
    d_branch = d_resid_one.astype(jnp.bfloat16)
    grad_out = contract_first(attended, d_branch)
    d_attended = (
        contract_last(d_branch, w_out).astype(jnp.bfloat16).reshape(slot_len, HEADS, HEAD_DIM)
    )
    d_query_blocks = []
    d_key_wide = jnp.zeros((slot_len, HEADS, HEAD_DIM), jnp.float32)
    d_value_wide = jnp.zeros((slot_len, HEADS, HEAD_DIM), jnp.float32)
    for block_number, first_row in enumerate(range(0, slot_len, block_len)):
        query_block, scores = block_scores(first_row)
        prob_full = jnp.exp(scores - lse_blocks[block_number])
        d_out_block = d_attended[first_row : first_row + block_len]
        d_value_wide = d_value_wide + jnp.einsum(
            "hqk,qhd->khd",
            prob_full.astype(jnp.bfloat16),
            d_out_block,
            preferred_element_type=jnp.float32,
        )
        d_prob = jnp.einsum(
            "qhd,khd->hqk", d_out_block, value_wide, preferred_element_type=jnp.float32
        )
        d_scores = (
            prob_full * (d_prob - jnp.sum(d_prob * prob_full, axis=-1, keepdims=True))
        ).astype(jnp.bfloat16)
        d_query_blocks.append(
            jnp.einsum("hqk,khd->qhd", d_scores, key_wide, preferred_element_type=jnp.float32)
            * 0.125
        )
        d_key_wide = (
            d_key_wide
            + jnp.einsum("hqk,qhd->khd", d_scores, query_block, preferred_element_type=jnp.float32)
            * 0.125
        )
    d_queries = rotate(jnp.concatenate(d_query_blocks, axis=0), cos_rows, sin_rows, -1.0)
    d_keys = rotate(
        d_key_wide.reshape(slot_len, KV_HEADS, group_size, HEAD_DIM).sum(axis=2),
        cos_rows,
        sin_rows,
        -1.0,
    )
    d_values = d_value_wide.reshape(slot_len, KV_HEADS, group_size, HEAD_DIM).sum(axis=2)
    d_mixed = jnp.concatenate(
        [
            d_queries.reshape(slot_len, model_width),
            d_keys.reshape(slot_len, kv_width),
            d_values.reshape(slot_len, kv_width),
        ],
        axis=1,
    ).astype(jnp.bfloat16)
    grad_qkv = contract_first(normed_one, d_mixed)
    d_normed_one = contract_last(d_mixed, w_qkv)
    d_embed_norm, d_gain_one = norm_back(embedded, gains_full[0], d_normed_one)
    d_embedded = (d_resid_one + d_embed_norm).astype(jnp.bfloat16)
    grad_gains = jnp.stack([d_gain_one, d_gain_two, d_gain_three], axis=0)
    gain_note = jnp.pad(
        grad_gains.reshape(-1), (0, note_shape[0] * 128 - 3 * model_width)
    ).reshape(note_shape)

    def give(turn):
        rows_out = contract_first(take_hot(turn), d_embedded)
        landed, notes = deal_rows(
            rows_out.astype(jnp.bfloat16).reshape(device_count, deal_cap, model_width),
            gain_note,
            sizes,
            2,
            "deal_rows",
        )
        return (
            contract_first(
                send_hot(turn), landed.reshape(device_count * deal_cap, model_width)
            ),
            notes,
        )

    d_table_tokens, gain_notes = give(0)
    grad_table = lax.fori_loop(
        1, rounds, lambda turn, held: held + give(turn)[0], d_table_head + d_table_tokens
    )
    gain_total = (
        jnp.sum(gain_notes, axis=0).reshape(-1)[: 3 * model_width].reshape(3, model_width)
    )
    gain_width = norm_gains.shape[1]
    own_grads = tuple(
        lax.psum(
            lax.psum_scatter(
                gradient.astype(jnp.bfloat16), "shard", scatter_dimension=0, tiled=True
            ),
            "dp",
        ).astype(jnp.float32)
        for gradient in (grad_qkv, grad_out, grad_gate_up, grad_down)
    ) + (lax.dynamic_slice_in_dim(gain_total, shard_me * gain_width, gain_width, 1),)
    layer_squares = sum((jnp.sum(gradient * gradient) for gradient in own_grads))
    layer_squares = jnp.where(dp_me == 0, layer_squares, 0.0)
    table_squares = jnp.sum(grad_table * grad_table)
    squares_all = gather_all(
        jnp.broadcast_to(layer_squares + table_squares, (8, 128)), sizes, 6, "gather_squares"
    )
    grad_norm = jnp.sqrt(jnp.sum(squares_all[:, 0, 0]))
    factor = max_norm / jnp.maximum(grad_norm, max_norm)
    firsts = (attend_in_first, attend_out_first, feed_in_first, feed_out_first, norm_gains_first)
    seconds = (
        attend_in_second,
        attend_out_second,
        feed_in_second,
        feed_out_second,
        norm_gains_second,
    )
    decays = (1.0, 1.0, 1.0, 1.0, 0.0)
    updated = [
        adamw_update(
            masters[number],
            firsts[number],
            seconds[number],
            own_grads[number] * factor,
            decays[number],
        )
        for number in range(5)
    ]
    table_new, table_first, table_second, _ = adamw_update(
        embed_table, embed_table_first, embed_table_second, grad_table * factor, 1.0
    )
    return (
        updated[0][0],
        updated[1][0],
        updated[2][0],
        updated[3][0],
        updated[4][3],
        table_new,
        updated[0][1],
        updated[1][1],
        updated[2][1],
        updated[3][1],
        updated[4][1],
        table_first,
        updated[0][2],
        updated[1][2],
        updated[2][2],
        updated[3][2],
        updated[4][2],
        table_second,
        mean_loss,
        grad_norm,
        seq_loss,
    )


def solution(mesh):
    in_specs = (
        P(("dp", "shard"), None),
        P(("dp", "shard")),
        P(("dp", "shard"), None),
        P(("dp", "shard")),
        P("shard", None),
        P("shard", None),
        P("shard", None),
        P("shard", None),
        P(None, "shard"),
        P(("dp", "shard"), None),
        P("shard", None),
        P("shard", None),
        P("shard", None),
        P("shard", None),
        P(None, "shard"),
        P(("dp", "shard"), None),
        P("shard", None),
        P("shard", None),
        P("shard", None),
        P("shard", None),
        P(None, "shard"),
        P(("dp", "shard"), None),
    )
    out_specs = (
        P("shard", None),
        P("shard", None),
        P("shard", None),
        P("shard", None),
        P(None, "shard"),
        P(("dp", "shard"), None),
        P("shard", None),
        P("shard", None),
        P("shard", None),
        P("shard", None),
        P(None, "shard"),
        P(("dp", "shard"), None),
        P("shard", None),
        P("shard", None),
        P("shard", None),
        P("shard", None),
        P(None, "shard"),
        P(("dp", "shard"), None),
        P(),
        P(),
        P(("dp", "shard")),
    )
    return jax.shard_map(
        per_device, mesh=mesh, in_specs=in_specs, out_specs=out_specs, check_vma=False
    )
```

```python
import functools

import jax
import jax.numpy as jnp
import numpy as np
from jax import lax
from jax.experimental import pallas as pl
from jax.experimental.pallas import tpu as pltpu
from jax.sharding import PartitionSpec as P


MESH = pl.DeviceIdType.MESH
VMEM = pltpu.MemorySpace.VMEM

HEADS = 15
KV_HEADS = 5
HEAD_DIM = 64
COMP = 16
STEP = 3


eps_norm = 1e-05
rope_base = 100000.0
beta_one = 0.5
beta_two = 0.5
adam_eps = 1e-08
learn_rate = 0.008
weight_decay = 0.1
max_norm = 0.01
masked_score = -1e30


def bits_of(size):
    return [1 << bit for bit in reversed(range(size.bit_length() - 1))]


def routes_of(sizes, count):
    dp_stages = [(0, bit) for bit in bits_of(sizes[0])]
    shard_stages = [(1, bit) for bit in bits_of(sizes[1])]
    swapped = shard_stages[1:2] + shard_stages[:1] + shard_stages[2:]
    return [dp_stages + shard_stages, dp_stages + swapped][:count]


def place_of(me, route):
    return sum((me[axis] // bit) % 2 * (1 << number) for number, (axis, bit) in enumerate(route))


def partner_of(me, axis, bit):
    other = list(me)
    other[axis] = me[axis] + bit - 2 * bit * ((me[axis] // bit) % 2)
    return tuple(other)


def here():
    return (lax.axis_index("dp"), lax.axis_index("shard"))


def greet_partners(me, route):
    barrier = pltpu.get_barrier_semaphore()
    for axis, bit in route:
        pl.semaphore_signal(
            barrier, inc=1, device_id=partner_of(me, axis, bit), device_id_type=MESH
        )
    pl.semaphore_wait(barrier, len(route))


def gather_kernel(routes, x_ref, out_ref, send_sem, recv_sem, own_sem):
    me = here()
    greet_partners(me, routes[0])
    places = [place_of(me, route) for route in routes]
    owns = [
        pltpu.make_async_copy(x_ref.at[lane], out_ref.at[lane, place], own_sem.at[lane])
        for lane, place in enumerate(places)
    ]
    for own in owns:
        own.start()
    for own in owns:
        own.wait()
    for number in range(len(routes[0])):
        span = 1 << number
        sent = []
        for lane, place in enumerate(places):
            blocks = out_ref.at[lane, pl.ds(place // span * span, span)]
            copy = pltpu.make_async_remote_copy(
                src_ref=blocks,
                dst_ref=blocks,
                send_sem=send_sem.at[lane, number],
                recv_sem=recv_sem.at[lane, number],
                device_id=partner_of(me, *routes[lane][number]),
                device_id_type=MESH,
            )
            copy.start()
            sent.append(copy)
        for copy in sent:
            copy.wait()


def gather_all(blocks, sizes, collective_id, name):
    lanes = blocks.shape[0]
    routes = routes_of(sizes, lanes)
    count = len(routes[0])
    return pl.pallas_call(
        functools.partial(gather_kernel, routes),
        name=name,
        out_shape=jax.ShapeDtypeStruct(
            (lanes, sizes[0] * sizes[1]) + blocks.shape[1:], blocks.dtype
        ),
        in_specs=[pl.BlockSpec(memory_space=VMEM)],
        out_specs=pl.BlockSpec(memory_space=VMEM),
        scratch_shapes=[
            pltpu.SemaphoreType.DMA((lanes, count)),
            pltpu.SemaphoreType.DMA((lanes, count)),
            pltpu.SemaphoreType.DMA((lanes,)),
        ],
        compiler_params=pltpu.CompilerParams(collective_id=collective_id, has_side_effects=True),
    )(blocks)


def scatter_kernel(routes, x_ref, out_ref, total_ref, landed, send_sem, recv_sem):
    me = here()
    greet_partners(me, routes[0])
    places = [place_of(me, route) for route in routes]
    last = len(routes[0]) - 1
    base = 0

    for number in reversed(range(last + 1)):
        span = 1 << number
        source = x_ref if number == last else total_ref
        sent = []
        for lane, place in enumerate(places):
            parent = 0 if number == last else place // (2 * span) * (2 * span)
            mine = place // span * span
            other = mine + span - 2 * span * ((mine // span) % 2)
            copy = pltpu.make_async_remote_copy(
                src_ref=source.at[lane, pl.ds(other - parent, span)],
                dst_ref=landed.at[lane, pl.ds(base, span)],
                send_sem=send_sem.at[lane, number],
                recv_sem=recv_sem.at[lane, number],
                device_id=partner_of(me, *routes[lane][number]),
                device_id_type=MESH,
            )
            copy.start()
            sent.append((copy, mine - parent))
        for lane, (copy, kept) in enumerate(sent):
            copy.wait()
            result = source[lane, pl.ds(kept, span)] + landed[lane, base : base + span]
            if number:
                total_ref[lane, pl.ds(0, span)] = result
            else:
                out_ref[lane] = result[0]
        base += span


def scatter_all(blocks, sizes, collective_id, name):
    lanes, total = blocks.shape[:2]
    routes = routes_of(sizes, lanes)
    count = len(routes[0])
    return pl.pallas_call(
        functools.partial(scatter_kernel, routes),
        name=name,
        out_shape=jax.ShapeDtypeStruct((lanes,) + blocks.shape[2:], blocks.dtype),
        in_specs=[pl.BlockSpec(memory_space=VMEM)],
        out_specs=pl.BlockSpec(memory_space=VMEM),
        scratch_shapes=[
            pltpu.VMEM((lanes, total // 2) + blocks.shape[2:], blocks.dtype),
            pltpu.VMEM((lanes, total) + blocks.shape[2:], blocks.dtype),
            pltpu.SemaphoreType.DMA((lanes, count)),
            pltpu.SemaphoreType.DMA((lanes, count)),
        ],
        compiler_params=pltpu.CompilerParams(collective_id=collective_id, has_side_effects=True),
    )(blocks)


def deal_kernel(
    sizes, rows_ref, note_ref, out_ref, notes_ref, send_sem, recv_sem, note_send, note_recv, own_sem
):
    total = sizes[0] * sizes[1]
    dp_at, shard_at = here()
    me = dp_at * sizes[1] + shard_at
    barrier = pltpu.get_barrier_semaphore()

    def peer_at(step):
        peer = lax.rem(me + step, total)
        return peer, (peer // sizes[1], peer % sizes[1])

    @pl.loop(1, total)
    def _(step):
        pl.semaphore_signal(barrier, inc=1, device_id=peer_at(step)[1], device_id_type=MESH)

    own = pltpu.make_async_copy(rows_ref.at[me], out_ref.at[me], own_sem.at[0])
    own.start()
    own_note = pltpu.make_async_copy(note_ref, notes_ref.at[me], own_sem.at[1])
    own_note.start()
    pl.semaphore_wait(barrier, total - 1)

    def copies(step):
        peer, device = peer_at(step)
        return (
            pltpu.make_async_remote_copy(
                src_ref=note_ref,
                dst_ref=notes_ref.at[me],
                send_sem=note_send.at[peer],
                recv_sem=note_recv.at[me],
                device_id=device,
                device_id_type=MESH,
            ),
            pltpu.make_async_remote_copy(
                src_ref=rows_ref.at[peer],
                dst_ref=out_ref.at[me],
                send_sem=send_sem.at[peer],
                recv_sem=recv_sem.at[me],
                device_id=device,
                device_id_type=MESH,
            ),
        )

    @pl.loop(1, total)
    def _(step):
        for copy in copies(step):
            copy.start()

    own.wait()
    own_note.wait()

    @pl.loop(1, total)
    def _(step):
        peer, device = peer_at(step)
        for copy in copies(step):
            copy.wait_send()
        pltpu.make_async_remote_copy(
            src_ref=note_ref,
            dst_ref=notes_ref.at[peer],
            send_sem=note_send.at[peer],
            recv_sem=note_recv.at[peer],
            device_id=device,
            device_id_type=MESH,
        ).wait_recv()
        pltpu.make_async_remote_copy(
            src_ref=rows_ref.at[peer],
            dst_ref=out_ref.at[peer],
            send_sem=send_sem.at[peer],
            recv_sem=recv_sem.at[peer],
            device_id=device,
            device_id_type=MESH,
        ).wait_recv()


def deal_rows(rows, note, sizes, collective_id, name):
    total = sizes[0] * sizes[1]
    return pl.pallas_call(
        functools.partial(deal_kernel, sizes),
        name=name,
        out_shape=(
            jax.ShapeDtypeStruct(rows.shape, rows.dtype),
            jax.ShapeDtypeStruct((total,) + note.shape, note.dtype),
        ),
        in_specs=[pl.BlockSpec(memory_space=VMEM)] * 2,
        out_specs=(pl.BlockSpec(memory_space=VMEM),) * 2,
        scratch_shapes=[pltpu.SemaphoreType.DMA((total,))] * 4 + [pltpu.SemaphoreType.DMA((2,))],
        compiler_params=pltpu.CompilerParams(collective_id=collective_id, has_side_effects=True),
    )(rows, note)


def count_kernel(high_count, high_ref, low_ref, out_ref):
    high_pad = out_ref.shape[1]

    @pl.loop(0, high_ref.shape[0])
    def _(n):
        length = high_ref.shape[2]
        high_hot = (
            lax.broadcasted_iota(jnp.int32, (high_pad, length), 0) == high_ref[n]
        ).astype(jnp.float32)
        low_hot = (lax.broadcasted_iota(jnp.int32, (128, length), 0) == low_ref[n]).astype(
            jnp.float32
        )
        out_ref[n] = contract_last(high_hot.astype(jnp.bfloat16), low_hot.astype(jnp.bfloat16))


def count_rows(high, low, high_pad):
    count, length = high.shape
    return pl.pallas_call(
        functools.partial(count_kernel, high_pad),
        name="count_rows",
        out_shape=jax.ShapeDtypeStruct((count, high_pad, 128), jnp.float32),
        in_specs=[pl.BlockSpec(memory_space=VMEM)] * 2,
        out_specs=pl.BlockSpec(memory_space=VMEM),
    )(high.reshape(count, 1, length), low.reshape(count, 1, length))


def contract_last(left, right):
    return lax.dot_general(
        left, right, (((1,), (1,)), ((), ())), preferred_element_type=jnp.float32
    )


def contract_first(left, right):
    return lax.dot_general(
        left, right, (((0,), (0,)), ((), ())), preferred_element_type=jnp.float32
    )


def turn(rows, cos_rows, sin_rows, sign):
    half = rows.shape[0] // 2
    first_half, second_half = rows[:half], rows[half:]
    return jnp.concatenate(
        [
            first_half * cos_rows - sign * second_half * sin_rows,
            second_half * cos_rows + sign * first_half * sin_rows,
        ],
        axis=0,
    )


def key_range(first_len, query_at, block):
    return jnp.where(query_at * block >= first_len, first_len // block, 0)


def allowed_at(first_len, key_at, query_at, block):
    keys = key_at * block + lax.broadcasted_iota(jnp.int32, (block, block), 0)
    steps = query_at * block + lax.broadcasted_iota(jnp.int32, (1, block), 1)
    lowest = jnp.where(steps >= first_len, first_len, 0)
    return (keys <= steps) & (keys >= lowest)


def attend_kernel(
    block,
    len_ref,
    q_ref,
    k_ref,
    v_ref,
    cos_ref,
    sin_ref,
    out_ref,
    lse_ref,
    q_out,
    k_out,
    v_out,
    wide_ref,
    key_rows,
    held,
):
    first_len = len_ref[0]
    cos_rows, sin_rows = cos_ref[...], sin_ref[...]
    keys = turn(k_ref[0], cos_rows, sin_rows, 1.0).astype(jnp.bfloat16)
    k_out[0] = keys
    key_rows[...] = keys.T
    v_out[0] = v_ref[0].astype(jnp.bfloat16)
    heads, width, length = q_ref.shape
    for head in range(heads):
        queries = turn(q_ref[head], cos_rows, sin_rows, 1.0).astype(jnp.bfloat16)
        q_out[head] = queries * jnp.bfloat16(0.125)
    for query_at in range(length // block):
        at = pl.ds(query_at * block, block)
        first_key = key_range(first_len, query_at, block)

        def score(key_at, tops):
            start = pl.multiple_of(key_at * block, block)
            allowed = allowed_at(first_len, key_at, query_at, block)
            after = []
            for head in range(heads):
                scores = jnp.dot(
                    key_rows[pl.ds(start, block)],
                    q_out[head, :, at],
                    preferred_element_type=jnp.float32,
                )
                scores = jnp.where(allowed, scores, masked_score)
                held[head, pl.ds(start, block)] = scores
                after.append(
                    jnp.maximum(tops[head], jnp.max(scores.reshape(-1, 8, block), axis=0))
                )
            return tuple(after)

        tops = lax.fori_loop(
            first_key,
            query_at + 1,
            score,
            (jnp.full((8, block), masked_score, jnp.float32),) * heads,
        )
        tops = [jnp.max(top, axis=0, keepdims=True) for top in tops]

        def grow(key_at, totals):
            start = pl.multiple_of(key_at * block, block)
            after = []
            for head in range(heads):
                grown = jnp.exp(held[head, pl.ds(start, block)] - tops[head])
                held[head, pl.ds(start, block)] = grown
                after.append(totals[head] + jnp.sum(grown.reshape(-1, 8, block), axis=0))
            return tuple(after)

        totals = lax.fori_loop(
            first_key, query_at + 1, grow, (jnp.zeros((8, block), jnp.float32),) * heads
        )
        totals = [jnp.sum(total, axis=0, keepdims=True) for total in totals]
        shares = [1.0 / total for total in totals]

        def mix(key_at, mixed):
            start = pl.multiple_of(key_at * block, block)
            return tuple(
                mixed[head]
                + jnp.dot(
                    v_out[0, :, pl.ds(start, block)],
                    (held[head, pl.ds(start, block)] * shares[head]).astype(jnp.bfloat16),
                    preferred_element_type=jnp.float32,
                )
                for head in range(heads)
            )

        mixed = lax.fori_loop(
            first_key, query_at + 1, mix, (jnp.zeros((width, block), jnp.float32),) * heads
        )
        for head in range(heads):
            out_ref[head, :, at] = mixed[head].astype(jnp.bfloat16)
            wide_ref[head, :, at] = mixed[head]
            lse_ref[head, :, at] = tops[head] + jnp.log(totals[head])


def attend_back_kernel(
    block,
    len_ref,
    q_ref,
    k_ref,
    v_ref,
    o_ref,
    do_ref,
    lse_ref,
    cos_ref,
    sin_ref,
    dq_ref,
    dk_ref,
    dv_ref,
    key_rows,
    value_rows,
    query_rows,
    do_rows,
    dk_total,
    dv_total,
):
    first_len = len_ref[0]
    cos_rows, sin_rows = cos_ref[...], sin_ref[...]
    key_rows[...] = k_ref[0].T
    value_rows[...] = v_ref[0].T
    dk_total[...] = jnp.zeros_like(dk_total)
    dv_total[...] = jnp.zeros_like(dv_total)
    heads, width, length = q_ref.shape
    delta = []
    for head in range(heads):
        query_rows[head] = q_ref[head].T
        do_rows[head] = do_ref[head].T
        delta.append(
            jnp.sum(
                o_ref[head] * do_ref[head].astype(jnp.float32),
                axis=0,
                keepdims=True,
            )
        )
    for query_at in range(length // block):
        at = slice(query_at * block, (query_at + 1) * block)

        def step(key_at, held):
            start = pl.multiple_of(key_at * block, block)
            here_keys = pl.ds(start, block)
            allowed = allowed_at(first_len, key_at, query_at, block)
            after, d_value, d_key = [], 0.0, 0.0
            for head in range(heads):
                scores = jnp.dot(
                    key_rows[here_keys], q_ref[head, :, at], preferred_element_type=jnp.float32
                )
                probs = jnp.where(allowed, jnp.exp(scores - lse_ref[head, :, at]), 0.0)
                d_probs = jnp.dot(
                    value_rows[here_keys], do_ref[head, :, at], preferred_element_type=jnp.float32
                )
                d_scores = (probs * (d_probs - delta[head][:, at])).astype(jnp.bfloat16)
                d_value = d_value + jnp.dot(
                    probs.astype(jnp.bfloat16),
                    do_rows[head, at],
                    preferred_element_type=jnp.float32,
                )
                d_key = d_key + jnp.dot(
                    d_scores, query_rows[head, at], preferred_element_type=jnp.float32
                )
                after.append(
                    held[head]
                    + jnp.dot(
                        k_ref[0, :, here_keys], d_scores, preferred_element_type=jnp.float32
                    )
                )
            dv_total[here_keys] += d_value
            dk_total[here_keys] += d_key
            return tuple(after)

        ends = lax.fori_loop(
            key_range(first_len, query_at, block),
            query_at + 1,
            step,
            (jnp.zeros((width, block), jnp.float32),) * heads,
        )
        for head in range(heads):
            dq_ref[head, :, at] = turn(
                ends[head] * 0.125, cos_rows[:, at], sin_rows[:, at], -1.0
            ).astype(jnp.bfloat16)
    dk_ref[0] = turn(dk_total[...].T, cos_rows, sin_rows, -1.0).astype(jnp.bfloat16)
    dv_ref[0] = dv_total[...].T.astype(jnp.bfloat16)


def head_specs(length):
    share = HEADS // KV_HEADS

    def spec(count, offset=0):
        return pl.BlockSpec((count, HEAD_DIM, length), lambda g, n: (offset // count + g, 0, 0))

    wide = spec(share)
    narrow = spec(1)
    turns = pl.BlockSpec((HEAD_DIM // 2, length), lambda g, n: (0, 0))
    lse = pl.BlockSpec((share, 1, length), lambda g, n: (g, 0, 0))
    return spec, wide, narrow, turns, lse


def attend(mixed, first_len, cos_rows, sin_rows):
    length = mixed.shape[2]
    block = min(256, length)
    spec, wide, narrow, turns, lse = head_specs(length)
    shape = lambda count: jax.ShapeDtypeStruct((count, HEAD_DIM, length), jnp.bfloat16)
    pairs = KV_HEADS * (HEADS // KV_HEADS) * length * length
    return pl.pallas_call(
        functools.partial(attend_kernel, block),
        name="attend",
        grid_spec=pltpu.PrefetchScalarGridSpec(
            num_scalar_prefetch=1,
            grid=(KV_HEADS,),
            in_specs=[wide, spec(1, HEADS), spec(1, HEADS + KV_HEADS), turns, turns],
            out_specs=[wide, lse, wide, narrow, narrow, wide],
            scratch_shapes=[
                pltpu.VMEM((length, HEAD_DIM), jnp.bfloat16),
                pltpu.VMEM((HEADS // KV_HEADS, length, block), jnp.float32),
            ],
        ),
        out_shape=(
            shape(HEADS),
            jax.ShapeDtypeStruct((HEADS, 1, length), jnp.float32),
            shape(HEADS),
            shape(KV_HEADS),
            shape(KV_HEADS),
            jax.ShapeDtypeStruct((HEADS, HEAD_DIM, length), jnp.float32),
        ),
        cost_estimate=pl.CostEstimate(
            flops=2 * pairs * HEAD_DIM, bytes_accessed=12 << 20, transcendentals=pairs // 2
        ),
    )(first_len, mixed, mixed, mixed, cos_rows, sin_rows)


def attend_back(saved, d_out, first_len, cos_rows, sin_rows):
    _, lse_rows, queries, key_heads, value_heads, out = saved
    length = out.shape[2]
    block = min(256, length)
    _, wide, narrow, turns, lse = head_specs(length)
    shape = lambda count: jax.ShapeDtypeStruct((count, HEAD_DIM, length), jnp.bfloat16)
    rows = pltpu.VMEM((length, HEAD_DIM), jnp.bfloat16)
    wide_rows = pltpu.VMEM((HEADS // KV_HEADS, length, HEAD_DIM), jnp.bfloat16)
    totals = pltpu.VMEM((length, HEAD_DIM), jnp.float32)
    pairs = KV_HEADS * (HEADS // KV_HEADS) * length * length
    return pl.pallas_call(
        functools.partial(attend_back_kernel, block),
        name="attend_back",
        grid_spec=pltpu.PrefetchScalarGridSpec(
            num_scalar_prefetch=1,
            grid=(KV_HEADS,),
            in_specs=[wide, narrow, narrow, wide, wide, lse, turns, turns],
            out_specs=[wide, narrow, narrow],
            scratch_shapes=[rows, rows, wide_rows, wide_rows, totals, totals],
        ),
        out_shape=(shape(HEADS), shape(KV_HEADS), shape(KV_HEADS)),
        cost_estimate=pl.CostEstimate(
            flops=5 * pairs * HEAD_DIM, bytes_accessed=14 << 20, transcendentals=pairs // 2
        ),
    )(first_len, queries, key_heads, value_heads, out, d_out, lse_rows, cos_rows, sin_rows)


def rms_scale(rows_in):
    return lax.rsqrt(jnp.mean(rows_in * rows_in, axis=-1, keepdims=True) + eps_norm)


def norm_back(rows_in, gain_row, incoming):
    scale_rows = rms_scale(rows_in)
    weighted = incoming * gain_row
    d_rows = scale_rows * weighted - rows_in * (scale_rows * scale_rows * scale_rows) * jnp.mean(
        weighted * rows_in, axis=-1, keepdims=True
    )
    return (d_rows, jnp.sum(incoming * rows_in * scale_rows, axis=0))


def rotation(positions):
    half_dim = HEAD_DIM // 2
    freqs = rope_base ** (-jnp.arange(half_dim, dtype=jnp.float32) * 2.0 / HEAD_DIM)
    angles = freqs[:, None] * positions[None, :]
    return (jnp.cos(angles), jnp.sin(angles))


def adamw_update(master, first_old, second_old, gradient, decay_on):
    first_new = beta_one * first_old + (1.0 - beta_one) * gradient
    second_new = beta_two * second_old + (1.0 - beta_two) * gradient * gradient
    first_hat = first_new / (1.0 - beta_one**STEP)
    second_hat = second_new / (1.0 - beta_two**STEP)
    change = -learn_rate * (
        first_hat / (jnp.sqrt(second_hat) + adam_eps) + decay_on * weight_decay * master
    )
    return (master + change, first_new, second_new, change)


def per_device(
    token_ids,
    seq_lengths,
    completion_mask,
    deal,
    attend_in,
    attend_out,
    feed_in,
    feed_out,
    norm_gains,
    embed_table,
    attend_in_first,
    attend_out_first,
    feed_in_first,
    feed_out_first,
    norm_gains_first,
    embed_table_first,
    attend_in_second,
    attend_out_second,
    feed_in_second,
    feed_out_second,
    norm_gains_second,
    embed_table_second,
):
    shard_count = lax.axis_size("shard")
    group_count = lax.axis_size("dp")
    sizes = (group_count, shard_count)
    device_count = shard_count * group_count
    dp_me, shard_me = here()
    device_me = dp_me * shard_count + shard_me
    total_rows = 2 * COMP * device_count
    slot_len = token_ids.shape[1]
    model_width = attend_out.shape[1]
    masters = (attend_in, attend_out, feed_in, feed_out, norm_gains)
    copies = tuple((master.astype(jnp.bfloat16) for master in masters[:4]))
    head_width = attend_in.shape[1]
    out_at = -(-head_width // 128) * 128
    w_attend = lax.all_gather(
        jnp.concatenate([jnp.pad(copies[0], ((0, 0), (0, out_at - head_width))), copies[1]], axis=1),
        "shard",
        axis=0,
        tiled=True,
    )
    w_qkv, w_out = w_attend[:, :head_width], w_attend[:, out_at:]
    w_gate_up, w_down = (
        lax.all_gather(copies[2], "shard", axis=0, tiled=True),
        lax.all_gather(copies[3], "shard", axis=0, tiled=True),
    )
    table_rows = embed_table.astype(jnp.bfloat16)
    rows_dev = embed_table.shape[0]
    gain_width = norm_gains.shape[1]
    ff_width = w_down.shape[0]
    row_count = 2 * COMP

    side = jnp.concatenate(
        [
            seq_lengths[:, None],
            deal[:, None],
            jnp.zeros((token_ids.shape[0], 126), jnp.int32),
        ],
        axis=1,
    )
    seqs_all = gather_all(
        jnp.concatenate([token_ids * 2 + completion_mask, side], axis=1)[None],
        sizes,
        1,
        "gather_ids",
    )
    seqs_all = seqs_all.reshape(-1, slot_len + 128)
    lengths_all = seqs_all[:, slot_len]
    places_all = seqs_all[:, slot_len + 1]
    order = sorted(
        ((dp_at, shard_at) for dp_at in range(group_count) for shard_at in range(shard_count)),
        key=lambda at: place_of(at, routes_of(sizes, 1)[0]),
    )
    seqs_dev = token_ids.shape[0]
    group_of = jnp.asarray(np.repeat([at[0] for at in order], seqs_dev).astype(np.int32))
    buffer_of = group_of * shard_count + places_all // 2
    step_ids = jnp.arange(slot_len, dtype=jnp.int32)

    def own_row(half):
        hit = (group_of == dp_me) & (places_all == 2 * shard_me + half)
        return jnp.sum(jnp.where(hit[:, None], seqs_all, 0), axis=0)

    front_row, back_row = own_row(0), own_row(1)
    first_len = front_row[slot_len]
    front_slot = front_row[:slot_len]
    packed = jnp.where(
        step_ids < first_len,
        lax.dynamic_slice_in_dim(
            jnp.concatenate([front_slot, front_slot]), slot_len - first_len, slot_len
        ),
        back_row[:slot_len],
    )
    own_ids = packed // 2
    own_marks = packed % 2
    marks_before = jnp.sum(
        jnp.where(step_ids[None, :] <= step_ids[:, None], own_marks[None, :], 0), axis=1
    )
    chosen_hot = (
        marks_before[None, :] == 1 + jnp.arange(row_count, dtype=jnp.int32)[:, None]
    ) & (own_marks[None, :] == 1)
    own_targets = jnp.sum(jnp.where(chosen_hot, jnp.roll(own_ids, -1)[None, :], 0), axis=1)
    segment = (step_ids >= first_len).astype(jnp.int32)
    cos_rows, sin_rows = rotation((step_ids - segment * first_len).astype(jnp.float32))

    deal_cap = -(-5 * slot_len // (4 * device_count) // 8) * 8
    ids_all = seqs_all[:, :slot_len] // 2
    near = ids_all - device_me * rows_dev
    wanted = (
        (near >= 0)
        & (near < rows_dev)
        & (step_ids[None, :] >= slot_len - lengths_all[:, None])
    )
    high_count = -(-rows_dev // 128)
    high_pad = -(-high_count // 8) * 8
    seen = count_rows(
        jnp.where(wanted, near // 128, -1), jnp.where(wanted, near % 128, -1), high_pad
    )[:, :high_count]
    buffer_hot = (
        buffer_of[None, :] == jnp.arange(device_count, dtype=jnp.int32)[:, None]
    ).astype(jnp.float32)
    seen_by = (
        jnp.einsum("bn,nhl->bhl", buffer_hot, jnp.minimum(seen, 1.0)) > 0.5
    ).astype(jnp.float32)
    upto = (jnp.arange(128)[:, None] <= jnp.arange(128)[None, :]).astype(jnp.float32)
    within = jnp.einsum("bhl,lm->bhm", seen_by, upto)
    whole = within[:, :, -1]
    before = (jnp.arange(high_count)[:, None] < jnp.arange(high_count)[None, :]).astype(jnp.float32)
    rank_by = within + jnp.einsum("bh,hg->bg", whole, before)[:, :, None]
    rank_by = jnp.where(seen_by > 0.5, rank_by, 0.0).reshape(device_count, -1)[:, :rows_dev]

    owner = own_ids // rows_dev
    same_id = own_ids[None, :] == own_ids[:, None]
    is_first = (
        jnp.sum(jnp.where(same_id & (step_ids[None, :] < step_ids[:, None]), 1, 0), axis=1) == 0
    )
    rank_own = jnp.sum(
        jnp.where(
            is_first[None, :]
            & (owner[None, :] == owner[:, None])
            & (own_ids[None, :] < own_ids[:, None]),
            1,
            0,
        ),
        axis=1,
    )
    rounds_own = jnp.max(rank_own) // deal_cap + 1

    def send_hot(turn):
        spots = (turn * deal_cap + 1 + jnp.arange(deal_cap, dtype=jnp.int32)).astype(jnp.float32)
        return (
            (rank_by[:, None, :] == spots[None, :, None])
            .astype(jnp.bfloat16)
            .reshape(device_count * deal_cap, rows_dev)
        )

    def take_hot(turn):
        slot = rank_own - turn * deal_cap
        inside = (slot >= 0) & (slot < deal_cap)
        spot = jnp.where(inside, owner * deal_cap + slot, -1)
        return (
            spot[:, None] == jnp.arange(device_count * deal_cap, dtype=jnp.int32)[None, :]
        ).astype(jnp.bfloat16)

    def fetch(turn, note):
        rows_out = jnp.dot(send_hot(turn), table_rows, preferred_element_type=jnp.float32)
        landed, notes = deal_rows(
            rows_out.astype(jnp.bfloat16).reshape(device_count, deal_cap, model_width),
            note,
            sizes,
            2,
            "deal_rows",
        )
        found = jnp.dot(
            take_hot(turn),
            landed.reshape(device_count * deal_cap, model_width),
            preferred_element_type=jnp.float32,
        )
        return found, notes

    note_shape = (-(-(3 * model_width + row_count) // 1024) * 8, 128)
    first_note = jnp.concatenate(
        [
            rounds_own.astype(jnp.float32)[None],
            lax.reduce_precision(norm_gains, 8, 7).reshape(-1),
            jnp.zeros((note_shape[0] * 128 - 3 * gain_width - 1,), jnp.float32),
        ]
    ).reshape(note_shape)
    embedded, first_notes = fetch(0, first_note)
    first_notes = first_notes.reshape(device_count, -1)
    rounds = jnp.max(first_notes[:, 0]).astype(jnp.int32)
    gains_full = (
        first_notes[:shard_count, 1 : 1 + 3 * gain_width]
        .reshape(shard_count, 3, gain_width)
        .transpose(1, 0, 2)
        .reshape(3, model_width)
    )
    embedded = lax.fori_loop(
        1,
        rounds,
        lambda turn, held: held + fetch(turn, jnp.zeros(note_shape, jnp.float32))[0],
        embedded,
    )
    normed_one = (embedded * rms_scale(embedded) * gains_full[0]).astype(jnp.bfloat16)
    mixed = lax.dot_general(
        w_qkv, normed_one, (((0,), (1,)), ((), ())), preferred_element_type=jnp.float32
    )
    head_count = HEADS + 2 * KV_HEADS
    len_row = first_len.reshape(1)
    saved = attend(
        mixed.reshape(head_count, HEAD_DIM, slot_len), len_row, cos_rows, sin_rows
    )
    attended = saved[0].reshape(model_width, slot_len).T
    resid_one = embedded + jnp.dot(attended, w_out, preferred_element_type=jnp.float32)
    normed_two = (resid_one * rms_scale(resid_one) * gains_full[1]).astype(jnp.bfloat16)
    gate_up = jnp.dot(normed_two, w_gate_up, preferred_element_type=jnp.float32)
    gate_part = gate_up[:, :ff_width]
    up_part = gate_up[:, ff_width:]
    hidden = (jax.nn.silu(gate_part) * up_part).astype(jnp.bfloat16)
    resid_two = resid_one + jnp.dot(hidden, w_down, preferred_element_type=jnp.float32)
    final_rows = (resid_two * rms_scale(resid_two) * gains_full[2]).astype(jnp.bfloat16)
    chosen_rows = chosen_hot.astype(jnp.bfloat16)
    picked = jnp.dot(chosen_rows, final_rows, preferred_element_type=jnp.float32)
    wide = -(-(model_width + 2) // 128) * 128
    tagged = jnp.concatenate(
        [
            picked,
            (own_targets // 256).astype(jnp.float32)[:, None],
            (own_targets % 256).astype(jnp.float32)[:, None],
            jnp.zeros((row_count, wide - model_width - 2), jnp.float32),
        ],
        axis=1,
    ).astype(jnp.bfloat16)
    tagged_all = gather_all(tagged.reshape(2, COMP, wide), sizes, 3, "gather_rows").reshape(
        total_rows, wide
    )
    rows_all = tagged_all[:, :model_width]
    targets_all = tagged_all[:, model_width].astype(jnp.int32) * 256 + tagged_all[
        :, model_width + 1
    ].astype(jnp.int32)
    logits = contract_last(rows_all, table_rows)
    top_logit = jnp.max(logits, axis=1)
    sum_exp = jnp.sum(jnp.exp(logits - top_logit[:, None]), axis=1)
    stats = gather_all(
        jnp.concatenate([top_logit, sum_exp]).reshape(1, 2 * total_rows // 128, 128),
        sizes,
        4,
        "gather_stats",
    ).reshape(device_count, 2, total_rows)
    top_all = jnp.max(stats[:, 0], axis=0)
    lse_all = top_all + jnp.log(
        jnp.sum(stats[:, 1] * jnp.exp(stats[:, 0] - top_all[None, :]), axis=0)
    )
    target_hot = (targets_all - device_me * rows_dev)[:, None] == jnp.arange(
        rows_dev, dtype=jnp.int32
    )[None, :]
    d_logits = (
        (jnp.exp(logits - lse_all[:, None]) - target_hot.astype(jnp.float32)) / total_rows
    ).astype(jnp.bfloat16)
    d_picked = scatter_all(
        jnp.dot(d_logits, table_rows, preferred_element_type=jnp.float32).reshape(
            2, device_count, COMP, model_width
        ),
        sizes,
        5,
        "scatter_rows",
    ).reshape(row_count, model_width)
    lse_own = jnp.concatenate(
        [
            lax.dynamic_slice_in_dim(
                lse_all.reshape(2, device_count * COMP)[lane],
                place_of((dp_me, shard_me), route) * COMP,
                COMP,
            )
            for lane, route in enumerate(routes_of(sizes, 2))
        ]
    )
    target_rows = jnp.dot(
        jnp.roll(chosen_rows, 1, axis=1),
        embedded.astype(jnp.bfloat16),
        preferred_element_type=jnp.float32,
    )
    losses_own = lse_own - jnp.sum(picked * target_rows, axis=1)
    d_final = lax.dot_general(
        chosen_hot.astype(jnp.float32),
        d_picked,
        (((0,), (0,)), ((), ())),
        precision=lax.Precision.HIGHEST,
        preferred_element_type=jnp.float32,
    )
    d_resid_two, d_gain_three = norm_back(resid_two, gains_full[2], d_final)
    d_down = d_resid_two.astype(jnp.bfloat16)
    grad_down = contract_first(hidden, d_down).astype(jnp.bfloat16)
    reduced_down = lax.psum_scatter(grad_down, "shard", scatter_dimension=0, tiled=True)
    _, d_down = lax.optimization_barrier((grad_down, d_down))
    d_hidden = contract_last(d_down, w_down).astype(jnp.bfloat16).astype(jnp.float32)
    gate_sigmoid = jax.nn.sigmoid(gate_part)
    d_gate = d_hidden * up_part * gate_sigmoid * (1.0 + gate_part * (1.0 - gate_sigmoid))
    d_up = d_hidden * jax.nn.silu(gate_part)
    d_gate_up = jnp.concatenate([d_gate, d_up], axis=1).astype(jnp.bfloat16)
    grad_gate_up = contract_first(normed_two, d_gate_up).astype(jnp.bfloat16)
    reduced_gate_up = lax.psum_scatter(grad_gate_up, "shard", scatter_dimension=0, tiled=True)
    _, d_gate_up = lax.optimization_barrier((grad_gate_up, d_gate_up))
    d_normed_two = contract_last(d_gate_up, w_gate_up)
    d_resid_norm, d_gain_two = norm_back(resid_one, gains_full[1], d_normed_two)
    d_resid_one = d_resid_two + d_resid_norm
    d_branch = d_resid_one.astype(jnp.bfloat16)
    grad_out = contract_first(attended, d_branch).astype(jnp.bfloat16)
    _, d_branch = lax.optimization_barrier((grad_out, d_branch))
    d_attended = (
        lax.dot_general(
            w_out, d_branch, (((1,), (1,)), ((), ())), preferred_element_type=jnp.float32
        )
        .astype(jnp.bfloat16)
        .reshape(HEADS, HEAD_DIM, slot_len)
    )
    d_mixed = (
        jnp.concatenate(attend_back(saved, d_attended, len_row, cos_rows, sin_rows), axis=0)
        .reshape(head_count * HEAD_DIM, slot_len)
        .T
    )
    grad_qkv = contract_first(normed_one, d_mixed).astype(jnp.bfloat16)
    _, d_mixed = lax.optimization_barrier((grad_qkv, d_mixed))
    grad_attend = jnp.concatenate(
        [jnp.pad(grad_qkv, ((0, 0), (0, out_at - head_width))), grad_out], axis=1
    )
    grad_attend, reduced_gate_up = lax.optimization_barrier((grad_attend, reduced_gate_up))
    reduced_attend = lax.psum_scatter(grad_attend, "shard", scatter_dimension=0, tiled=True)
    d_normed_one = contract_last(d_mixed, w_qkv)
    d_embed_norm, d_gain_one = norm_back(embedded, gains_full[0], d_normed_one)
    d_embedded = (d_resid_one + d_embed_norm).astype(jnp.bfloat16)
    grad_gains = jnp.stack([d_gain_one, d_gain_two, d_gain_three], axis=0)
    last_note = jnp.concatenate(
        [
            grad_gains.reshape(-1),
            losses_own,
            jnp.zeros((note_shape[0] * 128 - 3 * model_width - row_count,), jnp.float32),
        ]
    ).reshape(note_shape)

    def give(turn):
        rows_out = contract_first(take_hot(turn), d_embedded)
        landed, notes = deal_rows(
            rows_out.astype(jnp.bfloat16).reshape(device_count, deal_cap, model_width),
            last_note,
            sizes,
            2,
            "deal_rows",
        )
        return (
            contract_first(
                send_hot(turn), landed.reshape(device_count * deal_cap, model_width)
            ),
            notes,
        )

    d_table_tokens, last_notes = give(0)
    last_notes = last_notes.reshape(device_count, -1)
    loss_rows = last_notes[:, 3 * model_width : 3 * model_width + row_count].reshape(
        device_count, 2, COMP
    )
    mean_loss = jnp.sum(loss_rows) / total_rows
    seq_means = jnp.mean(loss_rows, axis=2).reshape(-1)
    loss_at = (dp_me * shard_count + deal // 2) * 2 + deal % 2
    seq_loss = jnp.sum(
        jnp.where(
            loss_at[:, None] == jnp.arange(2 * device_count, dtype=jnp.int32)[None, :],
            seq_means[None, :],
            0.0,
        ),
        axis=1,
    )
    d_table_head = contract_first(d_logits, rows_all)
    grad_table = lax.fori_loop(
        1, rounds, lambda turn, held: held + give(turn)[0], d_table_head + d_table_tokens
    )
    gain_total = jnp.sum(last_notes, axis=0)[: 3 * model_width].reshape(3, model_width)
    summed_attend, summed_gate_up, summed_down = (
        summed.astype(jnp.float32)
        for summed in lax.psum((reduced_attend, reduced_gate_up, reduced_down), "dp")
    )
    own_grads = (
        summed_attend[:, :head_width],
        summed_attend[:, out_at:],
        summed_gate_up,
        summed_down,
    ) + (lax.dynamic_slice_in_dim(gain_total, shard_me * gain_width, gain_width, 1),)
    layer_squares = sum((jnp.sum(gradient * gradient) for gradient in own_grads))
    layer_squares = jnp.where(dp_me == 0, layer_squares, 0.0)
    table_squares = jnp.sum(grad_table * grad_table)
    squares_all = gather_all(
        jnp.broadcast_to(layer_squares + table_squares, (1, 8, 128)), sizes, 6, "gather_squares"
    )
    grad_norm = jnp.sqrt(jnp.sum(squares_all[0, :, 0, 0]))
    factor = max_norm / jnp.maximum(grad_norm, max_norm)
    firsts = (attend_in_first, attend_out_first, feed_in_first, feed_out_first, norm_gains_first)
    seconds = (
        attend_in_second,
        attend_out_second,
        feed_in_second,
        feed_out_second,
        norm_gains_second,
    )
    decays = (1.0, 1.0, 1.0, 1.0, 0.0)
    updated = [
        adamw_update(
            masters[number],
            firsts[number],
            seconds[number],
            own_grads[number] * factor,
            decays[number],
        )
        for number in range(5)
    ]
    table_new, table_first, table_second, _ = adamw_update(
        embed_table, embed_table_first, embed_table_second, grad_table * factor, 1.0
    )
    return (
        updated[0][0],
        updated[1][0],
        updated[2][0],
        updated[3][0],
        updated[4][3],
        table_new,
        updated[0][1],
        updated[1][1],
        updated[2][1],
        updated[3][1],
        updated[4][1],
        table_first,
        updated[0][2],
        updated[1][2],
        updated[2][2],
        updated[3][2],
        updated[4][2],
        table_second,
        mean_loss,
        grad_norm,
        seq_loss,
    )


def solution(mesh):
    in_specs = (
        P(("dp", "shard"), None),
        P(("dp", "shard")),
        P(("dp", "shard"), None),
        P(("dp", "shard")),
        P("shard", None),
        P("shard", None),
        P("shard", None),
        P("shard", None),
        P(None, "shard"),
        P(("dp", "shard"), None),
        P("shard", None),
        P("shard", None),
        P("shard", None),
        P("shard", None),
        P(None, "shard"),
        P(("dp", "shard"), None),
        P("shard", None),
        P("shard", None),
        P("shard", None),
        P("shard", None),
        P(None, "shard"),
        P(("dp", "shard"), None),
    )
    out_specs = (
        P("shard", None),
        P("shard", None),
        P("shard", None),
        P("shard", None),
        P(None, "shard"),
        P(("dp", "shard"), None),
        P("shard", None),
        P("shard", None),
        P("shard", None),
        P("shard", None),
        P(None, "shard"),
        P(("dp", "shard"), None),
        P("shard", None),
        P("shard", None),
        P("shard", None),
        P("shard", None),
        P(None, "shard"),
        P(("dp", "shard"), None),
        P(),
        P(),
        P(("dp", "shard")),
    )
    return jax.shard_map(
        per_device, mesh=mesh, in_specs=in_specs, out_specs=out_specs, check_vma=False
    )
```
